32 devices in a mesh: cx: 4 (over y, x), cy: 8 (over z, core).
Axes of the slice: x: 2, y: 2, z: 4, core: 2. Of those that a mesh axis runs over, the one named last changes fastest.
Arguments:
- queries: bfloat16 [7, 2048, 128], P(None, ('cx', 'cy')), may hold values from -8 to 8, as said below
- keys: bfloat16 [2048, 128], P(('cx', 'cy')), may hold values from -40 to 40, as said below
- values: bfloat16 [2048, 128], P(('cx', 'cy')), may hold values from -6 to 6
Outputs:
- attended: bfloat16 [7, 2048, 128], P(None, ('cx', 'cy'))
The draws below stay inside these ranges and needn't reach their ends.
Inputs may be any that keep to these rules, and one draw needn't show every extreme that they name: `queries`: every query is noise of about unit size in each entry plus one common direction of length 4, the same for all heads and tokens. The keys of the first four prompt positions carry a large component along the queries' common direction, so they draw much of every query's attention; all other keys are noise of about unit size in each entry.
All inputs are finite; a program needn't handle non-finite values.
Results may differ from the reference program's by a relative error of at most 0.001.
Values may be sent and summed in bfloat16 or wider, within the bound.
A program may use at most 192 MiB of HBM per device.

```python
import math
import jax
import jax.numpy as jnp
from jax import lax

HEAD = 128
GROUP = 7
TOK_DEV = 64
SEQ = 2048


def sink_direction(key):
    sample = jax.random.normal(jax.random.fold_in(key, 3), (HEAD,), jnp.float32)
    return sample / jnp.sqrt(jnp.sum(sample * sample))


def noise_field(key, shape):
    return jnp.clip(jax.random.normal(key, shape, jnp.float32), -4.0, 4.0)


def draw_queries(key, part):
    direction = sink_direction(key)
    noise = noise_field(jax.random.fold_in(key, 1), (GROUP, SEQ, HEAD))
    return (noise + 4.0 * direction).astype(jnp.bfloat16)


def draw_keys(key, part):
    direction = sink_direction(key)
    noise = noise_field(jax.random.fold_in(key, 2), (SEQ, HEAD))
    lift = math.sqrt(HEAD) * (math.log(SEQ) - 1.0) / 4.0
    sinks = (jnp.arange(SEQ) < 4).astype(jnp.float32)
    return (noise + lift * sinks[:, None] * direction[None, :]).astype(jnp.bfloat16)


def block_scale(own_key, dims, shards, least, top_value):
    def one(position, parts):
        heights = jax.random.uniform(jax.random.fold_in(jax.random.fold_in(own_key, 6), position), (parts,), jnp.float32, least / len(shards), top_value / len(shards))
        return jnp.repeat(jnp.exp(heights), dims[position] // parts).reshape((-1,) + (1,) * (len(dims) - position - 1))

    level = one(*shards[0])
    for cut in shards[1:]:
        level = level * one(*cut)
    return level


def normal_values(rng, shape, spread, reach, pieces=(), kind=jnp.bfloat16):
    values = spread * jax.random.normal(rng, shape, jnp.float32)
    if pieces:
        values = values * block_scale(rng, shape, pieces, -0.22, 0.18)
    return jnp.clip(values, -reach, reach).astype(kind)


def setup_inputs(seed: int = 0) -> dict:
    key_of = jax.random.split(jax.random.key(seed), 4)
    return {
        "queries": draw_queries(jax.random.fold_in(key_of[3], 71), 0),
        "keys": draw_keys(jax.random.fold_in(key_of[3], 71), 0),
        "values": normal_values(key_of[2], (SEQ, HEAD), 1.0, 6.0, ((0, 32),)),
    }


masked = -1e30


def reference(queries, keys, values):
    key_pos = jnp.arange(SEQ, dtype=jnp.int32)
    values_wide = values.astype(jnp.float32)

    def row_block(number):
        first = (number * TOK_DEV).astype(jnp.int32)
        chosen = lax.dynamic_slice_in_dim(queries, first, TOK_DEV, 1).reshape(GROUP * TOK_DEV, HEAD)
        query_pos = first + jnp.arange(GROUP * TOK_DEV, dtype=jnp.int32) % TOK_DEV
        scores = jnp.dot(chosen, keys.T, preferred_element_type=jnp.float32) * (HEAD ** -0.5)
        visible = key_pos[None, :] <= query_pos[:, None]
        scores = jnp.where(visible, scores, masked)
        peak = jnp.max(scores, axis=1, keepdims=True)
        weights = jnp.where(visible, jnp.exp(scores - peak), 0.0)
        total = jnp.sum(weights, axis=1, keepdims=True)
        mixed = jnp.dot(weights, values_wide, precision=lax.Precision.HIGHEST)
        return (mixed / total).astype(jnp.bfloat16).reshape(GROUP, TOK_DEV, HEAD)

    blocks = lax.map(row_block, jnp.arange(SEQ // TOK_DEV, dtype=jnp.int32))
    return jnp.transpose(blocks, (1, 0, 2, 3)).reshape(GROUP, SEQ, HEAD)
```

```python
import functools

import jax
import jax.numpy as jnp
from jax import lax
from jax.experimental import pallas as pl
from jax.experimental.pallas import tpu as pltpu
from jax.sharding import PartitionSpec as P

MESH = pl.DeviceIdType.MESH
LOG2E = 1.4426950408889634
CORES = 2
SPAN = 8


def kernel(
    rows_n, line_n, queries_hbm, keys_hbm, values_hbm, out_ref,
    queries, kv, peak, total, mixed,
    in_sems, line_send, column_send, cross_send, mate_send, recv_sems,
):
    group, tokens, head = queries.shape
    count = group * tokens
    chips = line_n // CORES
    row = lax.axis_index("cx")
    place = lax.axis_index("cy")
    z, core = place // CORES, place % CORES
    mine = row * line_n + place
    cross_row = rows_n - 1 - row

    def block_id(r, zz, cc):
        return r * line_n + zz * CORES + cc

    def remote(block, sem, r, y):
        return pltpu.make_async_remote_copy(
            src_ref=kv.at[block], dst_ref=kv.at[block], send_sem=sem, recv_sem=recv_sems.at[block],
            device_id=(r, y), device_id_type=MESH,
        )

    def place_of(zz):
        return zz * CORES + core

    mate = z * CORES + 1 - core

    def to_line(block, sem, zz):
        return remote(block, sem, row, place_of(zz))

    def to_row(block, sem, r):
        return remote(block, sem, r, place)

    def to_mate(block):
        return remote(block, mate_send.at[block], row, mate)

    def arrived(block):
        to_mate(block).wait_recv()

    load_k = pltpu.make_async_copy(keys_hbm, kv.at[mine, 0], in_sems.at[0])
    load_v = pltpu.make_async_copy(values_hbm, kv.at[mine, 1], in_sems.at[1])
    load_q = pltpu.make_async_copy(queries_hbm, queries, in_sems.at[2])
    load_k.start()
    load_v.start()
    load_q.start()

    barrier = pltpu.get_barrier_semaphore()

    def greet_line(i, _):
        @pl.when(i != z)
        def _():
            pl.semaphore_signal(barrier, inc=1, device_id=(row, place_of(i)), device_id_type=MESH)
        return 0

    def greet_column(i, _):
        @pl.when(i != row)
        def _():
            pl.semaphore_signal(barrier, inc=1, device_id=(i, place), device_id_type=MESH)
        return 0

    lax.fori_loop(0, chips, greet_line, 0)
    lax.fori_loop(0, rows_n, greet_column, 0)
    pl.semaphore_signal(barrier, inc=1, device_id=(row, mate), device_id_type=MESH)
    load_k.wait()
    load_v.wait()
    pl.semaphore_wait(barrier, chips - 1 + rows_n - 1 + 1)

    def around(body):
        def step(d, _):
            @pl.when(z + d < chips)
            def _():
                body(z + d)

            @pl.when(z - d >= 0)
            def _():
                body(z - d)
            return 0

        lax.fori_loop(1, chips, step, 0)

    def later_rows(body):
        def step(r, _):
            body(r)
            return 0

        lax.fori_loop(row + 1, rows_n, step, 0)

    last_row = row == rows_n - 1
    has_cross = cross_row < row

    def send_own(zz):
        @pl.when(jnp.logical_or(zz > z, row < rows_n - 1))
        def _():
            to_line(mine, line_send.at[zz], zz).start()

    around(send_own)
    later_rows(lambda r: to_row(mine, column_send.at[r * chips + z], r).start())

    @pl.when(core == 0)
    def _():
        to_mate(mine).start()

    load_q.wait()
    scale = head ** (-0.5) * LOG2E

    def scores_of(first, blocks):
        k = kv[pl.ds(first, blocks), 0].reshape(blocks * tokens, head)
        q = queries[...].reshape(count, head)
        return lax.dot_general(q, k, (((1,), (1,)), ((), ())), preferred_element_type=jnp.float32)

    def mix(weights, first, blocks):
        v = kv[pl.ds(first, blocks), 1].reshape(blocks * tokens, head)
        high = weights.astype(jnp.bfloat16)
        low = (weights - high.astype(jnp.float32)).astype(jnp.bfloat16)
        return jnp.dot(high, v, preferred_element_type=jnp.float32) + jnp.dot(
            low, v, preferred_element_type=jnp.float32
        )

    def fold(first, blocks):
        scores = scores_of(first, blocks)
        old = peak[...]
        fresh = jnp.maximum(old, jnp.max(scores, axis=1, keepdims=True))
        shrink = jnp.exp2((old - fresh) * scale)
        weights = jnp.exp2((scores - fresh[:, :1]) * scale)
        peak[...] = fresh
        total[...] = total[...] * shrink + jnp.sum(weights, axis=1, keepdims=True)
        mixed[...] = mixed[...] * shrink + mix(weights, first, blocks)

    scores = scores_of(mine, 1)
    query_pos = lax.broadcasted_iota(jnp.int32, (count, tokens), 0) % tokens
    key_pos = lax.broadcasted_iota(jnp.int32, (count, tokens), 1)
    visible = key_pos <= query_pos
    scores = jnp.where(visible, scores, -1e30)
    top = jnp.max(scores, axis=1, keepdims=True)
    weights = jnp.where(visible, jnp.exp2((scores - top) * scale), 0.0)
    peak[...] = jnp.broadcast_to(top, peak.shape)
    total[...] = jnp.broadcast_to(jnp.sum(weights, axis=1, keepdims=True), total.shape)
    mixed[...] = mix(weights, mine, 1)

    def pass_own_row(zz):
        @pl.when(jnp.logical_or(zz < z, row < rows_n - 1))
        def _():
            block = block_id(row, zz, core)
            arrived(block)

            def on(r):
                @pl.when(r != cross_row)
                def _():
                    to_row(block, column_send.at[r * chips + zz], r).start()

            later_rows(on)

            @pl.when(zz < z)
            def _():
                to_mate(block).start()

    def pass_cross():
        block = block_id(cross_row, z, core)
        arrived(block)
        around(lambda zz: to_line(block, cross_send.at[zz], zz).start())
        to_mate(block).start()

    @pl.when(has_cross)
    def _():
        pass_cross()

    around(pass_own_row)

    @pl.when(core == 1)
    def _():
        block = block_id(row, z, 0)
        arrived(block)
        fold(block, 1)

    def own_row_step(zz, _):
        arrived(block_id(row, zz, 1 - core))
        fold(block_id(row, zz, 0), CORES)
        return 0

    lax.fori_loop(0, z, own_row_step, 0)

    def take_row(r):
        def step(zz):
            block = block_id(r, zz, core)
            arrived(block)
            to_mate(block).start()

        @pl.when(r != cross_row)
        def _():
            step(z)

        around(step)

    def fold_row(r):
        def wait_mate(zz, _):
            arrived(block_id(r, zz, 1 - core))
            return 0

        lax.fori_loop(0, chips, wait_mate, 0)
        span = min(SPAN, line_n)

        def part(i, _):
            fold(r * line_n + i * span, span)
            return 0

        lax.fori_loop(0, line_n // span, part, 0)

    def earlier(i, _):
        r = row - 1 - i
        take_row(r)
        fold_row(r)
        return 0

    lax.fori_loop(0, row, earlier, 0)

    out_ref[...] = (mixed[...] / total[...]).astype(out_ref.dtype).reshape(out_ref.shape)

    def sent_own(zz):
        @pl.when(jnp.logical_or(zz > z, row < rows_n - 1))
        def _():
            to_line(mine, line_send.at[zz], zz).wait_send()

        @pl.when(jnp.logical_or(zz < z, row < rows_n - 1))
        def _():
            block = block_id(row, zz, core)

            def on(r):
                @pl.when(r != cross_row)
                def _():
                    to_row(block, column_send.at[r * chips + zz], r).wait_send()

            later_rows(on)

            @pl.when(zz < z)
            def _():
                to_mate(block).wait_send()

        @pl.when(has_cross)
        def _():
            to_line(block_id(cross_row, z, core), cross_send.at[zz], zz).wait_send()

    around(sent_own)
    later_rows(lambda r: to_row(mine, column_send.at[r * chips + z], r).wait_send())

    @pl.when(core == 0)
    def _():
        to_mate(mine).wait_send()

    def sent_rows(r, _):
        def step(zz, _):
            to_mate(block_id(r, zz, core)).wait_send()
            return 0

        lax.fori_loop(0, chips, step, 0)
        return 0

    lax.fori_loop(0, row, sent_rows, 0)


def local(rows_n, line_n, queries, keys, values):
    group, tokens, head = queries.shape
    blocks = rows_n * line_n
    chips = line_n // CORES
    count = group * tokens
    return pl.pallas_call(
        functools.partial(kernel, rows_n, line_n),
        out_shape=jax.ShapeDtypeStruct(queries.shape, jnp.bfloat16),
        in_specs=[pl.BlockSpec(memory_space=pl.ANY)] * 3,
        out_specs=pl.BlockSpec(memory_space=pltpu.VMEM),
        scratch_shapes=[
            pltpu.VMEM(queries.shape, queries.dtype),
            pltpu.VMEM((blocks, 2, tokens, head), keys.dtype),
            pltpu.VMEM((count, head), jnp.float32),
            pltpu.VMEM((count, head), jnp.float32),
            pltpu.VMEM((count, head), jnp.float32),
            pltpu.SemaphoreType.DMA((3,)),
            pltpu.SemaphoreType.DMA((chips,)),
            pltpu.SemaphoreType.DMA((rows_n * chips,)),
            pltpu.SemaphoreType.DMA((chips,)),
            pltpu.SemaphoreType.DMA((blocks,)),
            pltpu.SemaphoreType.DMA((blocks,)),
        ],
        compiler_params=pltpu.CompilerParams(collective_id=0, has_side_effects=True),
    )(queries, keys, values)


def solution(mesh):
    rows_n, line_n = mesh.shape["cx"], mesh.shape["cy"]
    in_specs = (P(None, ("cx", "cy"), None), P(("cx", "cy"), None), P(("cx", "cy"), None))
    out_specs = P(None, ("cx", "cy"), None)
    return jax.shard_map(
        functools.partial(local, rows_n, line_n), mesh=mesh, in_specs=in_specs, out_specs=out_specs, check_vma=False
    )
```

```python
import functools

import jax
import jax.numpy as jnp
from jax import lax
from jax.experimental import pallas as pl
from jax.experimental.pallas import tpu as pltpu
from jax.sharding import PartitionSpec as P

MESH = pl.DeviceIdType.MESH
LOG2E = 1.4426950408889634
CORES = 2
SPAN = 8


def kernel(
    rows_n, line_n, queries_hbm, keys_hbm, values_hbm, out_ref,
    queries, kv, peak, total, mixed,
    in_sems, line_send, column_send, cross_send, mate_send, recv_sems,
):
    group, tokens, head = queries.shape
    count = group * tokens
    chips = line_n // CORES
    row = lax.axis_index("cx")
    place = lax.axis_index("cy")
    z, core = place // CORES, place % CORES
    mine = row * line_n + place
    cross_row = rows_n - 1 - row

    def block_id(r, zz, cc):
        return r * line_n + zz * CORES + cc

    def remote(block, sem, r, y):
        return pltpu.make_async_remote_copy(
            src_ref=kv.at[block], dst_ref=kv.at[block], send_sem=sem, recv_sem=recv_sems.at[block],
            device_id=(r, y), device_id_type=MESH,
        )

    def place_of(zz):
        return zz * CORES + core

    mate = z * CORES + 1 - core

    def to_line(block, sem, zz):
        return remote(block, sem, row, place_of(zz))

    def to_row(block, sem, r):
        return remote(block, sem, r, place)

    def to_mate(block):
        return remote(block, mate_send.at[block], row, mate)

    def arrived(block):
        to_mate(block).wait_recv()

    load_k = pltpu.make_async_copy(keys_hbm, kv.at[mine, 0], in_sems.at[0])
    load_v = pltpu.make_async_copy(values_hbm, kv.at[mine, 1], in_sems.at[1])
    load_q = pltpu.make_async_copy(queries_hbm, queries, in_sems.at[2])
    load_k.start()
    load_v.start()
    load_q.start()

    barrier = pltpu.get_barrier_semaphore()

    def greet_line(i, _):
        @pl.when(i != z)
        def _():
            pl.semaphore_signal(barrier, inc=1, device_id=(row, place_of(i)), device_id_type=MESH)
        return 0

    def greet_column(i, _):
        @pl.when(i != row)
        def _():
            pl.semaphore_signal(barrier, inc=1, device_id=(i, place), device_id_type=MESH)
        return 0

    lax.fori_loop(0, chips, greet_line, 0)
    lax.fori_loop(0, rows_n, greet_column, 0)
    pl.semaphore_signal(barrier, inc=1, device_id=(row, mate), device_id_type=MESH)
    load_k.wait()
    load_v.wait()
    pl.semaphore_wait(barrier, chips - 1 + rows_n - 1 + 1)

    def around(body, first=1, last=chips):
        def step(d, _):
            @pl.when(z + d < chips)
            def _():
                body(z + d)

            @pl.when(z - d >= 0)
            def _():
                body(z - d)
            return 0

        lax.fori_loop(first, last, step, 0)

    def later_rows(body):
        def step(r, _):
            body(r)
            return 0

        lax.fori_loop(row + 1, rows_n, step, 0)

    last_row = row == rows_n - 1
    has_cross = cross_row < row

    def send_own(zz):
        @pl.when(jnp.logical_or(zz > z, row < rows_n - 1))
        def _():
            to_line(mine, line_send.at[zz], zz).start()

    around(send_own)
    later_rows(lambda r: to_row(mine, column_send.at[r * chips + z], r).start())

    @pl.when(core == 0)
    def _():
        to_mate(mine).start()

    load_q.wait()
    scale = head ** (-0.5) * LOG2E

    def scores_of(first, blocks):
        k = kv[pl.ds(first, blocks), 0].reshape(blocks * tokens, head)
        q = queries[...].reshape(count, head)
        return lax.dot_general(q, k, (((1,), (1,)), ((), ())), preferred_element_type=jnp.float32)

    def mix(weights, first, blocks):
        v = kv[pl.ds(first, blocks), 1].reshape(blocks * tokens, head)
        high = weights.astype(jnp.bfloat16)
        low = (weights - high.astype(jnp.float32)).astype(jnp.bfloat16)
        return jnp.dot(high, v, preferred_element_type=jnp.float32) + jnp.dot(
            low, v, preferred_element_type=jnp.float32
        )

    def lane_sums(weights):
        width = weights.shape[1]
        if width % head:
            lane = lax.broadcasted_iota(jnp.int32, (count, head), 1)
            return jnp.where(lane == 0, jnp.sum(weights, axis=1, keepdims=True), 0.0)
        return sum(weights[:, i : i + head] for i in range(0, width, head))

    def fold(first, blocks):
        scores = scores_of(first, blocks)
        old = peak[...]
        fresh = jnp.maximum(old, jnp.max(scores, axis=1, keepdims=True))
        shrink = jnp.exp2((old - fresh) * scale)
        weights = jnp.exp2((scores - fresh[:, :1]) * scale)
        peak[...] = fresh
        total[...] = total[...] * shrink + lane_sums(weights)
        mixed[...] = mixed[...] * shrink + mix(weights, first, blocks)

    scores = scores_of(mine, 1)
    query_pos = lax.broadcasted_iota(jnp.int32, (count, tokens), 0) % tokens
    key_pos = lax.broadcasted_iota(jnp.int32, (count, tokens), 1)
    visible = key_pos <= query_pos
    scores = jnp.where(visible, scores, -1e30)
    top = jnp.max(scores, axis=1, keepdims=True)
    weights = jnp.where(visible, jnp.exp2((scores - top) * scale), 0.0)
    peak[...] = jnp.broadcast_to(top, peak.shape)
    total[...] = lane_sums(weights)
    mixed[...] = mix(weights, mine, 1)

    def pass_own_row(zz):
        @pl.when(jnp.logical_or(zz < z, row < rows_n - 1))
        def _():
            block = block_id(row, zz, core)
            arrived(block)

            def on(r):
                @pl.when(r != cross_row)
                def _():
                    to_row(block, column_send.at[r * chips + zz], r).start()

            later_rows(on)

            @pl.when(zz < z)
            def _():
                to_mate(block).start()

    def pass_cross():
        block = block_id(cross_row, z, core)
        arrived(block)
        around(lambda zz: to_line(block, cross_send.at[zz], zz).start())
        to_mate(block).start()

    around(pass_own_row, 1, 2)

    @pl.when(has_cross)
    def _():
        pass_cross()

    around(pass_own_row, 2, chips)

    def fold_own_row():
        @pl.when(core == 1)
        def _():
            block = block_id(row, z, 0)
            arrived(block)
            fold(block, 1)

        def own_row_step(zz, _):
            arrived(block_id(row, zz, 1 - core))
            fold(block_id(row, zz, 0), CORES)
            return 0

        lax.fori_loop(0, z, own_row_step, 0)

    def take_row(r):
        def step(zz):
            block = block_id(r, zz, core)
            arrived(block)
            to_mate(block).start()

        @pl.when(r != cross_row)
        def _():
            step(z)

        around(step)

    def fold_row(r):
        def wait_mate(zz, _):
            arrived(block_id(r, zz, 1 - core))
            return 0

        lax.fori_loop(0, chips, wait_mate, 0)
        span = min(SPAN, line_n)

        def part(i, _):
            fold(r * line_n + i * span, span)
            return 0

        lax.fori_loop(0, line_n // span, part, 0)

    def row_at(i):
        ahead = row - i
        passed = jnp.where(ahead <= cross_row, ahead - 1, ahead)
        return jnp.where(has_cross, jnp.where(i == 0, cross_row, passed), ahead - 1)

    @pl.when(row > 0)
    def _():
        take_row(row_at(0))

    fold_own_row()

    def earlier(i, _):
        take_row(row_at(i))
        fold_row(row_at(i - 1))
        return 0

    lax.fori_loop(1, row, earlier, 0)

    @pl.when(row > 0)
    def _():
        fold_row(row_at(row - 1))

    out_ref[...] = (mixed[...] / jnp.sum(total[...], axis=1, keepdims=True)).astype(out_ref.dtype).reshape(out_ref.shape)

    def sent_own(zz):
        @pl.when(jnp.logical_or(zz > z, row < rows_n - 1))
        def _():
            to_line(mine, line_send.at[zz], zz).wait_send()

        @pl.when(jnp.logical_or(zz < z, row < rows_n - 1))
        def _():
            block = block_id(row, zz, core)

            def on(r):
                @pl.when(r != cross_row)
                def _():
                    to_row(block, column_send.at[r * chips + zz], r).wait_send()

            later_rows(on)

            @pl.when(zz < z)
            def _():
                to_mate(block).wait_send()

        @pl.when(has_cross)
        def _():
            to_line(block_id(cross_row, z, core), cross_send.at[zz], zz).wait_send()

    around(sent_own)
    later_rows(lambda r: to_row(mine, column_send.at[r * chips + z], r).wait_send())

    @pl.when(core == 0)
    def _():
        to_mate(mine).wait_send()

    def sent_rows(r, _):
        def step(zz, _):
            to_mate(block_id(r, zz, core)).wait_send()
            return 0

        lax.fori_loop(0, chips, step, 0)
        return 0

    lax.fori_loop(0, row, sent_rows, 0)


def local(rows_n, line_n, queries, keys, values):
    group, tokens, head = queries.shape
    blocks = rows_n * line_n
    chips = line_n // CORES
    count = group * tokens
    return pl.pallas_call(
        functools.partial(kernel, rows_n, line_n),
        out_shape=pltpu.VMEM(queries.shape, jnp.bfloat16),
        in_specs=[pl.BlockSpec(memory_space=pltpu.HBM)] * 3,
        out_specs=pl.BlockSpec(memory_space=pltpu.VMEM),
        scratch_shapes=[
            pltpu.VMEM(queries.shape, queries.dtype),
            pltpu.VMEM((blocks, 2, tokens, head), keys.dtype),
            pltpu.VMEM((count, head), jnp.float32),
            pltpu.VMEM((count, head), jnp.float32),
            pltpu.VMEM((count, head), jnp.float32),
            pltpu.SemaphoreType.DMA((3,)),
            pltpu.SemaphoreType.DMA((chips,)),
            pltpu.SemaphoreType.DMA((rows_n * chips,)),
            pltpu.SemaphoreType.DMA((chips,)),
            pltpu.SemaphoreType.DMA((blocks,)),
            pltpu.SemaphoreType.DMA((blocks,)),
        ],
        compiler_params=pltpu.CompilerParams(collective_id=0, has_side_effects=True),
    )(queries, keys, values)


def solution(mesh):
    rows_n, line_n = mesh.shape["cx"], mesh.shape["cy"]
    in_specs = (P(None, ("cx", "cy"), None), P(("cx", "cy"), None), P(("cx", "cy"), None))
    out_specs = P(None, ("cx", "cy"), None)
    return jax.shard_map(
        functools.partial(local, rows_n, line_n), mesh=mesh, in_specs=in_specs, out_specs=out_specs, check_vma=False
    )
```

```python
import functools

import jax
import jax.numpy as jnp
from jax import lax
from jax.experimental import pallas as pl
from jax.experimental.pallas import tpu as pltpu
from jax.sharding import PartitionSpec as P

MESH = pl.DeviceIdType.MESH
LOG2E = 1.4426950408889634
CORES = 2
SPAN = 8


def kernel(
    rows_n, line_n, queries_hbm, keys_hbm, values_hbm, out_ref,
    queries, kv, peak, total, mixed,
    in_sems, line_send, column_send, cross_send, mate_send, recv_sems,
):
    group, tokens, head = queries.shape
    count = group * tokens
    chips = line_n // CORES
    row = lax.axis_index("cx")
    place = lax.axis_index("cy")
    z, core = place // CORES, place % CORES
    mine = row * line_n + place
    cross_row = rows_n - 1 - row

    def block_id(r, zz, cc):
        return r * line_n + zz * CORES + cc

    def remote(block, sem, r, y):
        return pltpu.make_async_remote_copy(
            src_ref=kv.at[block], dst_ref=kv.at[block], send_sem=sem, recv_sem=recv_sems.at[block],
            device_id=(r, y), device_id_type=MESH,
        )

    def place_of(zz):
        return zz * CORES + core

    mate = z * CORES + 1 - core

    def to_line(block, sem, zz):
        return remote(block, sem, row, place_of(zz))

    def to_row(block, sem, r):
        return remote(block, sem, r, place)

    def to_mate(block):
        return remote(block, mate_send.at[block], row, mate)

    def arrived(block):
        to_mate(block).wait_recv()

    load_k = pltpu.make_async_copy(keys_hbm, kv.at[mine, 0], in_sems.at[0])
    load_v = pltpu.make_async_copy(values_hbm, kv.at[mine, 1], in_sems.at[1])
    load_q = pltpu.make_async_copy(queries_hbm, queries, in_sems.at[2])

    barrier = pltpu.get_barrier_semaphore()

    def greet_line(i, _):
        @pl.when(i != z)
        def _():
            pl.semaphore_signal(barrier, inc=1, device_id=(row, place_of(i)), device_id_type=MESH)
        return 0

    def greet_column(i, _):
        @pl.when(i != row)
        def _():
            pl.semaphore_signal(barrier, inc=1, device_id=(i, place), device_id_type=MESH)
        return 0

    lax.fori_loop(0, chips, greet_line, 0)
    lax.fori_loop(0, rows_n, greet_column, 0)
    pl.semaphore_signal(barrier, inc=1, device_id=(row, mate), device_id_type=MESH)
    load_k.start()
    load_v.start()
    load_q.start()
    load_k.wait()
    load_v.wait()
    pl.semaphore_wait(barrier, chips - 1 + rows_n - 1 + 1)

    def around(body, first=1, last=chips):
        def step(d, _):
            @pl.when(z + d < chips)
            def _():
                body(z + d)

            @pl.when(z - d >= 0)
            def _():
                body(z - d)
            return 0

        lax.fori_loop(first, last, step, 0)

    def around_far_first(body):
        def step(i, _):
            d = chips - i

            @pl.when(z + d < chips)
            def _():
                body(z + d)

            @pl.when(z - d >= 0)
            def _():
                body(z - d)
            return 0

        lax.fori_loop(1, chips, step, 0)

    def later_rows(body):
        def step(r, _):
            body(r)
            return 0

        lax.fori_loop(row + 1, rows_n, step, 0)

    last_row = row == rows_n - 1
    has_cross = cross_row < row

    def send_own(zz):
        @pl.when(jnp.logical_or(zz > z, row < rows_n - 1))
        def _():
            to_line(mine, line_send.at[zz], zz).start()

    around_far_first(send_own)
    later_rows(lambda r: to_row(mine, column_send.at[r * chips + z], r).start())

    @pl.when(core == 0)
    def _():
        to_mate(mine).start()

    load_q.wait()
    scale = head ** (-0.5) * LOG2E

    def scores_of(first, blocks):
        k = kv[pl.ds(first, blocks), 0].reshape(blocks * tokens, head)
        q = queries[...].reshape(count, head)
        return lax.dot_general(q, k, (((1,), (1,)), ((), ())), preferred_element_type=jnp.float32)

    def mix(weights, first, blocks):
        v = kv[pl.ds(first, blocks), 1].reshape(blocks * tokens, head)
        high = weights.astype(jnp.bfloat16)
        low = (weights - high.astype(jnp.float32)).astype(jnp.bfloat16)
        return jnp.dot(high, v, preferred_element_type=jnp.float32) + jnp.dot(
            low, v, preferred_element_type=jnp.float32
        )

    def lane_sums(weights):
        width = weights.shape[1]
        if width % head:
            lane = lax.broadcasted_iota(jnp.int32, (count, head), 1)
            return jnp.where(lane == 0, jnp.sum(weights, axis=1, keepdims=True), 0.0)
        return sum(weights[:, i : i + head] for i in range(0, width, head))

    def fold(first, blocks):
        scores = scores_of(first, blocks)
        old = peak[...]
        fresh = jnp.maximum(old, jnp.max(scores, axis=1, keepdims=True))
        shrink = jnp.exp2((old - fresh) * scale)
        weights = jnp.exp2((scores - fresh[:, :1]) * scale)
        peak[...] = fresh
        total[...] = total[...] * shrink + lane_sums(weights)
        mixed[...] = mixed[...] * shrink + mix(weights, first, blocks)

    scores = scores_of(mine, 1)
    query_pos = lax.broadcasted_iota(jnp.int32, (count, tokens), 0) % tokens
    key_pos = lax.broadcasted_iota(jnp.int32, (count, tokens), 1)
    visible = key_pos <= query_pos
    scores = jnp.where(visible, scores, -1e30)
    top = jnp.max(scores, axis=1, keepdims=True)
    weights = jnp.where(visible, jnp.exp2((scores - top) * scale), 0.0)
    peak[...] = jnp.broadcast_to(top, peak.shape)
    total[...] = lane_sums(weights)
    mixed[...] = mix(weights, mine, 1)

    def pass_own_row(zz):
        @pl.when(jnp.logical_or(zz < z, row < rows_n - 1))
        def _():
            block = block_id(row, zz, core)
            arrived(block)

            def on(r):
                @pl.when(r != cross_row)
                def _():
                    to_row(block, column_send.at[r * chips + zz], r).start()

            later_rows(on)

            @pl.when(zz < z)
            def _():
                to_mate(block).start()

    def pass_cross():
        block = block_id(cross_row, z, core)
        arrived(block)
        around_far_first(lambda zz: to_line(block, cross_send.at[zz], zz).start())
        to_mate(block).start()

    around(pass_own_row, 1, 2)

    @pl.when(has_cross)
    def _():
        pass_cross()

    around(pass_own_row, 2, chips)

    def fold_own_row():
        @pl.when(core == 1)
        def _():
            block = block_id(row, z, 0)
            arrived(block)
            fold(block, 1)

        def own_row_step(zz, _):
            arrived(block_id(row, zz, 1 - core))
            fold(block_id(row, zz, 0), CORES)
            return 0

        lax.fori_loop(0, z, own_row_step, 0)

    halves = 2 if chips % 2 == 0 else 1
    stretch = chips // halves
    near = z // stretch

    def take(r, half):
        def step(zz):
            block = block_id(r, zz, core)
            arrived(block)
            to_mate(block).start()

        @pl.when(jnp.logical_and(r != cross_row, half == near))
        def _():
            step(z)

        def other(zz):
            @pl.when(zz // stretch == half)
            def _():
                step(zz)

        around(other)

    def fold_half(r, half):
        def wait_mate(i, _):
            arrived(block_id(r, half * stretch + i, 1 - core))
            return 0

        lax.fori_loop(0, stretch, wait_mate, 0)
        span = min(SPAN, stretch * CORES)

        def part(i, _):
            fold(block_id(r, half * stretch, 0) + i * span, span)
            return 0

        lax.fori_loop(0, stretch * CORES // span, part, 0)

    def row_at(i):
        ahead = row - i
        passed = jnp.where(ahead <= cross_row, ahead - 1, ahead)
        return jnp.where(has_cross, jnp.where(i == 0, cross_row, passed), ahead - 1)

    def each_row(body):
        def step(i, _):
            body(row_at(i))
            return 0

        lax.fori_loop(0, row, step, 0)

    each_row(lambda r: take(r, near))
    fold_own_row()
    each_row(lambda r: fold_half(r, near))
    if halves == 2:
        each_row(lambda r: take(r, 1 - near))
        each_row(lambda r: fold_half(r, 1 - near))

    out_ref[...] = (mixed[...] / jnp.sum(total[...], axis=1, keepdims=True)).astype(out_ref.dtype).reshape(out_ref.shape)

    def sent_own(zz):
        @pl.when(jnp.logical_or(zz > z, row < rows_n - 1))
        def _():
            to_line(mine, line_send.at[zz], zz).wait_send()

        @pl.when(jnp.logical_or(zz < z, row < rows_n - 1))
        def _():
            block = block_id(row, zz, core)

            def on(r):
                @pl.when(r != cross_row)
                def _():
                    to_row(block, column_send.at[r * chips + zz], r).wait_send()

            later_rows(on)

            @pl.when(zz < z)
            def _():
                to_mate(block).wait_send()

        @pl.when(has_cross)
        def _():
            to_line(block_id(cross_row, z, core), cross_send.at[zz], zz).wait_send()

    around(sent_own)
    later_rows(lambda r: to_row(mine, column_send.at[r * chips + z], r).wait_send())

    @pl.when(core == 0)
    def _():
        to_mate(mine).wait_send()

    def sent_rows(r, _):
        def step(zz, _):
            to_mate(block_id(r, zz, core)).wait_send()
            return 0

        lax.fori_loop(0, chips, step, 0)
        return 0

    lax.fori_loop(0, row, sent_rows, 0)


def local(rows_n, line_n, queries, keys, values):
    group, tokens, head = queries.shape
    blocks = rows_n * line_n
    chips = line_n // CORES
    count = group * tokens
    return pl.pallas_call(
        functools.partial(kernel, rows_n, line_n),
        out_shape=pltpu.VMEM(queries.shape, jnp.bfloat16),
        in_specs=[pl.BlockSpec(memory_space=pltpu.HBM)] * 3,
        out_specs=pl.BlockSpec(memory_space=pltpu.VMEM),
        scratch_shapes=[
            pltpu.VMEM(queries.shape, queries.dtype),
            pltpu.VMEM((blocks, 2, tokens, head), keys.dtype),
            pltpu.VMEM((count, head), jnp.float32),
            pltpu.VMEM((count, head), jnp.float32),
            pltpu.VMEM((count, head), jnp.float32),
            pltpu.SemaphoreType.DMA((3,)),
            pltpu.SemaphoreType.DMA((chips,)),
            pltpu.SemaphoreType.DMA((rows_n * chips,)),
            pltpu.SemaphoreType.DMA((chips,)),
            pltpu.SemaphoreType.DMA((blocks,)),
            pltpu.SemaphoreType.DMA((blocks,)),
        ],
        compiler_params=pltpu.CompilerParams(collective_id=0, has_side_effects=True),
    )(queries, keys, values)


def solution(mesh):
    rows_n, line_n = mesh.shape["cx"], mesh.shape["cy"]
    in_specs = (P(None, ("cx", "cy"), None), P(("cx", "cy"), None), P(("cx", "cy"), None))
    out_specs = P(None, ("cx", "cy"), None)
    return jax.shard_map(
        functools.partial(local, rows_n, line_n), mesh=mesh, in_specs=in_specs, out_specs=out_specs, check_vma=False
    )
```
